128 devices in a mesh: pipe: 4 (over y_hi, core), exp: 16 (over x, z), pair: 2 (over y_lo).
Axes of the slice: x: 4, y: 4 (y_hi: 2, y_lo: 2; y = y_hi * 2 + y_lo), z: 4, core: 2. Of those that a mesh axis runs over, the one named last changes fastest.
Arguments:
- hidden_in: bfloat16 [4, 1024, 2048], P(None, ('exp', 'pair')), may hold values from -6 to 6
- routes: int32 [4, 4, 1024, 8], P('pipe', None, ('exp', 'pair')), may hold values from 0 to 63, all different within a row; in each aligned block of 32 rows (0 to 31, 32 to 63, ..., all dimensions but the last counted through in order) at most 6 rows name the same one
- gate_probs: float32 [4, 4, 1024, 8], P('pipe', None, ('exp', 'pair')), may hold values from 0.02 to 1
- norm_gain: float32 [4, 2048], P('pipe'), may hold values from 0.1 to 1.9
- w_gate: bfloat16 [4, 64, 2048, 768], P('pipe', ('exp', 'pair')), may hold values from -0.125 to 0.125
- w_up: bfloat16 [4, 64, 2048, 768], P('pipe', ('exp', 'pair')), may hold values from -0.125 to 0.125
- w_down: bfloat16 [4, 64, 768, 2048], P('pipe', ('exp', 'pair')), may hold values from -0.21875 to 0.21875
Outputs:
- layer_outputs: bfloat16 [4, 4, 1024, 2048], P('pipe', None, ('exp', 'pair'))
The draws below stay inside these ranges and needn't reach their ends.
Inputs may be any that keep to these rules, and one draw needn't show every extreme that they name: `routes`: within each layer and micro-batch, the 32 tokens of one device (aligned blocks) name no expert more than 6 times in all, and each token names 8 different experts.
All inputs are finite; a program needn't handle non-finite values.
Results may differ from the reference program's by a relative error of at most 0.01.
Values may be sent and summed in bfloat16 or wider, within the bound.
A program may use at most 64 MiB of HBM per device.

```python
import math
import jax
import jax.numpy as jnp
import numpy as np
from jax import lax

D = 2048
FF = 768
TOPK = 8
MB = 4
TOK_DEV = 32
EXPERTS = 64
LAYERS = 4
TOKENS = 1024
CAP = 6


def block_scale(rng, shape, shards, least, largest):
    def one(position, parts):
        steps = jax.random.uniform(jax.random.fold_in(jax.random.fold_in(rng, 6), position), (parts,), jnp.float32, least / len(shards), largest / len(shards))
        return jnp.repeat(jnp.exp(steps), shape[position] // parts).reshape((-1,) + (1,) * (len(shape) - position - 1))

    loudness = one(*shards[0])
    for cut in shards[1:]:
        loudness = loudness * one(*cut)
    return loudness


def routed_block(rng, own, number, rows, number_of, top, bound, skew):
    order = jax.random.permutation(rng, number_of)
    packed, common = shares(number_of, rows * top, bound, skew, True), shares(number_of, rows * top, bound, skew, False)
    places = jnp.arange(number_of)

    def named(sizes, rotation):
        used = int((sizes > 0).sum())
        fixed = max(1, used // 4)
        shifted = fixed + (places - fixed + rotation * (used - fixed)) % max(1, number_of - fixed)
        return jnp.zeros((number_of,), jnp.int32).at[order[jnp.where(places < fixed, places, shifted)]].set(jnp.asarray(sizes, jnp.int32))

    sizes = jnp.where(number % 4 == 0, named(packed, number // 4), named(common, number - number // 4 - 1))
    mixed = jax.random.permutation(jax.random.fold_in(own, 3), number_of)
    donor, taker = mixed[0:number_of // 2 * 2:2], mixed[1:number_of // 2 * 2:2]
    margin = jnp.minimum(sizes[donor] - 1, bound - sizes[taker]) // 2
    margin = jnp.where((donor == order[0]) | (taker == order[0]) | (sizes[taker] == 0), 0, jnp.maximum(margin, 0))
    shifted = jax.random.randint(jax.random.fold_in(own, 4), (number_of // 2,), 0, 1 << 20) % (margin + 1)
    sizes = sizes.at[donor].add(-shifted).at[taker].add(shifted)
    labels = jnp.searchsorted(jnp.cumsum(sizes), jnp.arange(rows * top), side="right").astype(jnp.int32)
    grid = labels.reshape(top, rows).T
    grid = grid[jax.random.permutation(jax.random.fold_in(own, 1), rows)]
    rotation = jax.random.randint(jax.random.fold_in(own, 2), (rows, 1), 0, top)
    return jnp.take_along_axis(grid, (jnp.arange(top)[None, :] + rotation) % top, axis=1)


def shares(number_of, total, most, skew, full):
    loads = [(1 << 20) // math.isqrt(grade ** skew) + 1 for grade in range(1, number_of + 1)]
    largest = most if full else min(most, max(-(-total // number_of), total * loads[0] // sum(loads)))
    least = 1 if total - largest >= number_of - 1 else 0
    counts, surplus = [largest] + [least] * (number_of - 1), total - largest - least * (number_of - 1)
    while surplus > 0:
        candidates = [i for i in range(1, number_of) if counts[i] < largest] or [i for i in range(1, number_of) if counts[i] < most]
        mass, remaining = sum([loads[i] for i in candidates]), surplus
        for i in candidates:
            addition = min(most - counts[i], max(1, remaining * loads[i] // mass), surplus)
            counts[i] = counts[i] + addition
            surplus = surplus - addition
    return np.array(counts)


def normal_values(own_key, dims, width, most, shards=(), held_as=jnp.bfloat16):
    drawn = jax.random.normal(own_key, dims, jnp.float32) * width
    if len(shards) > 0:
        drawn = block_scale(own_key, dims, shards, -0.22, 0.18) * drawn
    return jnp.clip(drawn, min=-most, max=most).astype(held_as)


def setup_inputs(seed: int = 0) -> dict:
    key_of = jax.random.split(jax.random.key(seed), 8)
    hidden_in = normal_values(key_of[0], (MB, TOKENS, D), 1.0, 6.0, ((1, 32),))
    routes_keys = jax.random.split(jax.random.fold_in(key_of[1], 1), LAYERS * MB * TOKENS // TOK_DEV)
    routes_turns = jax.random.permutation(jax.random.fold_in(key_of[1], 3), LAYERS * MB * TOKENS // TOK_DEV)
    routes = jax.vmap(lambda own, number: routed_block(jax.random.fold_in(key_of[1], 2), own, number, TOK_DEV, EXPERTS, TOPK, CAP, 2))(routes_keys, routes_turns).reshape((LAYERS, MB, TOKENS, TOPK))
    gate_probs = jnp.clip(jnp.exp(math.log(1.0) - 3.912023 * jax.random.uniform(key_of[2], (LAYERS, MB, TOKENS, TOPK), jnp.float32) ** block_scale(key_of[2], (LAYERS, MB, TOKENS, TOPK), ((0, 4), (2, 32)), -0.2, 0.2)), 0.02, 1.0)
    norm_gain = jnp.clip(1.0 + 0.18 * jax.random.normal(key_of[3], (LAYERS, D), jnp.float32), 0.1, 1.9)
    w_gate = normal_values(key_of[4], (LAYERS, EXPERTS, D, FF), D ** -0.5, 0.125, ((0, 4), (1, 32)))
    w_up = normal_values(key_of[5], (LAYERS, EXPERTS, D, FF), D ** -0.5, 0.125, ((0, 4), (1, 32)))
    w_down = normal_values(key_of[6], (LAYERS, EXPERTS, FF, D), FF ** -0.5, 0.21875, ((0, 4), (1, 32)))
    return {"hidden_in": hidden_in, "routes": routes, "gate_probs": gate_probs, "norm_gain": norm_gain, "w_gate": w_gate, "w_up": w_up, "w_down": w_down}


EPS = 1e-06

def slots_of(block_routes):
    expert_ids = jnp.arange(EXPERTS, dtype=jnp.int32)
    onehot = (block_routes[:, None] == expert_ids[None, :]).astype(jnp.int32)
    before = jnp.cumsum(onehot, axis=0) - onehot
    return lax.optimization_barrier(jnp.sum(before * onehot, axis=1)).astype(jnp.int32)

def moe_layer(state, chosen, probs, gain, wgate, wupper, wdown):
    floated = state.astype(jnp.float32)
    scale = lax.rsqrt(lax.optimization_barrier(jnp.mean(floated * floated, axis=-1, keepdims=True)) + EPS)
    normed = (floated * scale * gain.astype(jnp.float32)).astype(jnp.bfloat16)
    blocks = TOKENS // TOK_DEV
    flat_routes = chosen.reshape(blocks, TOK_DEV * TOPK).astype(jnp.int32)
    slots = jax.vmap(slots_of)(flat_routes)
    columns = (slots + CAP * jnp.arange(blocks, dtype=jnp.int32)[:, None]).reshape(-1)
    rows_ids = flat_routes.reshape(-1)
    buffer = jnp.zeros((EXPERTS, blocks * CAP, D), jnp.bfloat16)
    buffer = buffer.at[rows_ids, columns].set(jnp.repeat(normed, TOPK, axis=0))

    def one_expert(items):
        inputs, gate_w, up_w, down_w = items
        gate = jnp.dot(inputs, gate_w, preferred_element_type=jnp.float32)
        upward = jnp.dot(inputs, up_w, preferred_element_type=jnp.float32)
        hidden = (jax.nn.silu(gate) * upward).astype(jnp.bfloat16)
        return jnp.dot(hidden, down_w, preferred_element_type=jnp.float32).astype(jnp.bfloat16)
    produced = lax.map(one_expert, (buffer, wgate, wupper, wdown))
    picked = produced[rows_ids, columns].reshape(TOKENS, TOPK, D).astype(jnp.float32)
    probs32 = probs.astype(jnp.float32)
    weights = probs32 / lax.optimization_barrier(jnp.sum(probs32, axis=-1, keepdims=True))
    mixed = jnp.einsum('tk,tkd->td', weights, picked)
    return (floated + mixed).astype(jnp.bfloat16)

def reference(hidden_in, routes, gate_probs, norm_gain, w_gate, w_up, w_down):
    current = hidden_in
    outputs = []
    for layer in range(LAYERS):

        def per_batch(items):
            state, chosen, probs = items
            return moe_layer(state, chosen, probs, norm_gain[layer], w_gate[layer], w_up[layer], w_down[layer])
        current = lax.map(per_batch, (current, routes[layer], gate_probs[layer]))
        outputs.append(current)
    return jnp.stack(outputs, axis=0)
```

```python
import functools

import jax
import jax.numpy as jnp
from jax import lax
from jax.experimental import pallas as pl
from jax.experimental.pallas import tpu as pltpu
from jax.sharding import PartitionSpec as P

EPS = 1e-06
MESH = pl.DeviceIdType.MESH
BF16 = jnp.bfloat16
F32 = jnp.float32
SIDE = 4
COLS = 256


def kernel(stages, groups, cap, hidden_ref, routes_ref, probs_ref, gain_ref, wg_hbm, wu_hbm, wd_hbm, out_ref,
           wg, wu, wd, send, recv, back, done, relay, state, normed, rows, hid, total, pick, mix,
           w_sem, d_send, d_recv, r_send, r_recv, n_send, n_recv):
    stage, exp, pair = lax.axis_index("pipe"), lax.axis_index("exp"), lax.axis_index("pair")
    pairs = lax.axis_size("pair")
    me = exp * pairs + pair
    micro, tok, width = hidden_ref.shape
    top = routes_ref.shape[2]
    local, _, slots, _ = send.shape[1:]
    span = groups * slots
    hidden_units = wg.shape[2]

    def weight_copies(e):
        return [pltpu.make_async_copy(hbm.at[e], vmem.at[e], w_sem.at[i, e])
                for i, (hbm, vmem) in enumerate(((wg_hbm, wg), (wu_hbm, wu), (wd_hbm, wd)))]

    for e in range(local):
        for copy in weight_copies(e):
            copy.start()

    barrier = pltpu.get_barrier_semaphore()

    def greet(i, carry):
        peer = lax.rem(me + i, groups)
        pl.semaphore_signal(barrier, inc=1, device_id=(stage, peer // pairs, lax.rem(peer, pairs)), device_id_type=MESH)
        return carry

    lax.fori_loop(1, groups, greet, 0)

    @pl.when(stage > 0)
    def _():
        pl.semaphore_signal(barrier, inc=1, device_id=(stage - 1, exp, pair), device_id_type=MESH)

    def prepare(m):
        column = lax.broadcasted_iota(jnp.int32, (tok, local * groups), 1)
        expert = lax.rem(column, groups) * local + column // groups
        probs = probs_ref[m]
        probs = probs / jnp.sum(probs, axis=-1, keepdims=True)
        routes = routes_ref[m]
        named = jnp.zeros((tok, local * groups), F32)
        weight = jnp.zeros((tok, local * groups), F32)
        for k in range(top):
            hit = routes[:, k:k + 1] == expert
            named = named + jnp.where(hit, 1.0, 0.0)
            weight = weight + jnp.where(hit, probs[:, k:k + 1], 0.0)
        earlier = lax.broadcasted_iota(jnp.int32, (tok, tok), 1) < lax.broadcasted_iota(jnp.int32, (tok, tok), 0)
        before = jnp.dot(jnp.where(earlier, 1.0, 0.0).astype(BF16), named.astype(BF16), preferred_element_type=F32)
        high = weight.astype(BF16)
        low = (weight - high.astype(F32)).astype(BF16)
        shape = (local * groups, local * span)
        spread = jnp.where(lax.broadcasted_iota(jnp.int32, shape, 1) // slots == lax.broadcasted_iota(jnp.int32, shape, 0), 1.0, 0.0)
        spread = spread.astype(BF16)
        slot = lax.rem(lax.broadcasted_iota(jnp.int32, (tok, local * span), 1), slots).astype(F32)
        taken = jnp.dot(named.astype(BF16), spread, preferred_element_type=F32)
        place = jnp.dot(before.astype(BF16), spread, preferred_element_type=F32)
        mask = jnp.logical_and(taken > 0.5, jnp.abs(place - slot) < 0.5)
        mix[m, 0:tok, :] = jnp.where(mask, jnp.dot(high, spread, preferred_element_type=F32), 0.0).astype(BF16)
        mix[m, tok:2 * tok, :] = jnp.where(mask, jnp.dot(low, spread, preferred_element_type=F32), 0.0).astype(BF16)
        pick[m] = jnp.where(mask, 1.0, 0.0).T.astype(BF16)

    prepare(0)
    pl.semaphore_wait(barrier, groups - 1 + jnp.minimum(stages - 1 - stage, 1))

    offsets = [(dx, dz, dy) for dx in range(SIDE) for dz in range(SIDE) for dy in range(2)][1:]

    def exchange(source, target, m, e, s_sem, r_sem):
        x, z = exp // SIDE, lax.rem(exp, SIDE)
        for dx, dz, dy in offsets:
            peer_exp = lax.rem(x + dx, SIDE) * SIDE + lax.rem(z + dz, SIDE)
            peer_pair = lax.rem(pair + dy, pairs)
            peer = peer_exp * pairs + peer_pair
            pltpu.make_async_remote_copy(
                src_ref=source.at[m, e, peer, pl.ds(0, cap)],
                dst_ref=target.at[m, e, me, pl.ds(0, cap)],
                send_sem=s_sem.at[m, e],
                recv_sem=r_sem.at[m, e],
                device_id=(stage, peer_exp, peer_pair),
                device_id_type=MESH,
            ).start()
        target[m, e, me] = source[m, e, me]

    def arrived(buffer, m, e, sem):
        part = buffer.at[m, e, pl.ds(0, groups - 1), pl.ds(0, cap)]
        pltpu.make_async_copy(part, part, sem.at[m, e]).wait()

    def relay_copy(m, target_stage):
        return pltpu.make_async_remote_copy(
            src_ref=out_ref.at[m], dst_ref=relay.at[m], send_sem=n_send.at[m], recv_sem=n_recv.at[m],
            device_id=(target_stage, exp, pair), device_id_type=MESH)

    def one(m, carry):
        @pl.when(stage == 0)
        def _():
            state[...] = hidden_ref[m].astype(F32)

        @pl.when(stage > 0)
        def _():
            relay_copy(m, stage).wait_recv()
            state[...] = relay[m].astype(F32)

        floated = state[...]
        scale = lax.rsqrt(jnp.mean(floated * floated, axis=-1, keepdims=True) + EPS)
        normed[...] = (floated * scale * gain_ref[...]).astype(BF16)

        def dispatch(e, carry):
            begin = pl.multiple_of(e * span, span)
            for c in range(0, width, COLS):
                made = jnp.dot(pick[m, pl.ds(begin, span), :], normed[:, c:c + COLS], preferred_element_type=F32)
                send[m, e, :, :, c:c + COLS] = made.reshape(groups, slots, COLS).astype(BF16)
            exchange(send, recv, m, e, d_send, d_recv)
            return carry

        lax.fori_loop(0, local, dispatch, 0)
        done[m, :, :, cap:slots, :] = jnp.zeros((local, groups, slots - cap, width), BF16)

        def ffn(e, carry):
            @pl.when(m == 0)
            def _():
                for copy in weight_copies(e):
                    copy.wait()

            arrived(recv, m, e, d_recv)
            rows[...] = recv[m, e].reshape(span, width)
            for c in range(0, hidden_units, COLS):
                gate = jnp.dot(rows[...], wg[e, :, c:c + COLS], preferred_element_type=F32)
                upward = jnp.dot(rows[...], wu[e, :, c:c + COLS], preferred_element_type=F32)
                hid[:, c:c + COLS] = (jax.nn.silu(gate) * upward).astype(BF16)
            for c in range(0, width, COLS):
                made = jnp.dot(hid[...], wd[e, :, c:c + COLS], preferred_element_type=F32)
                back[m, e, :, :, c:c + COLS] = made.reshape(groups, slots, COLS).astype(BF16)
            exchange(back, done, m, e, r_send, r_recv)
            return carry

        lax.fori_loop(0, local, ffn, 0)

        @pl.when(m + 1 < micro)
        def _():
            prepare(m + 1)

        total[...] = jnp.zeros_like(total)

        def combine(e, carry):
            arrived(done, m, e, r_recv)
            begin = pl.multiple_of(e * span, span)
            for c in range(0, width, COLS):
                total[:, c:c + COLS] += jnp.dot(mix[m, :, pl.ds(begin, span)],
                                                done[m, e, :, :, c:c + COLS].reshape(span, COLS), preferred_element_type=F32)
            return carry

        lax.fori_loop(0, local, combine, 0)
        out_ref[m] = (state[...] + (total[0:tok, :] + total[tok:2 * tok, :])).astype(BF16)

        @pl.when(stage < stages - 1)
        def _():
            relay_copy(m, stage + 1).start()

        return carry

    lax.fori_loop(0, micro, one, 0)

    def finish(m, carry):
        for e in range(local):
            arrived(send, m, e, d_send)
            arrived(back, m, e, r_send)

        @pl.when(stage < stages - 1)
        def _():
            relay_copy(m, stage + 1).wait_send()

        return carry

    lax.fori_loop(0, micro, finish, 0)


def solution(mesh):
    stages = mesh.shape["pipe"]
    groups = mesh.shape["exp"] * mesh.shape["pair"]

    def on_device(hidden_in, routes, gate_probs, norm_gain, w_gate, w_up, w_down):
        micro, tok, width = hidden_in.shape
        top = routes.shape[3]
        local, _, units = w_gate.shape[1:]
        experts = local * groups
        cap = max(2, 3 * tok * top // (2 * experts))
        slots = -(-cap // 8) * 8
        span = groups * slots
        vmem = pl.BlockSpec(memory_space=pltpu.VMEM)
        hbm = pl.BlockSpec(memory_space=pl.ANY)
        buffer = pltpu.VMEM((micro, local, groups, slots, width), BF16)
        sem = pltpu.SemaphoreType.DMA((micro, local))
        out = pl.pallas_call(
            functools.partial(kernel, stages, groups, cap),
            out_shape=jax.ShapeDtypeStruct((micro, tok, width), BF16),
            in_specs=[vmem] * 4 + [hbm] * 3,
            out_specs=vmem,
            scratch_shapes=[
                pltpu.VMEM((local, width, units), BF16),
                pltpu.VMEM((local, width, units), BF16),
                pltpu.VMEM((local, units, width), BF16),
                buffer, buffer, buffer, buffer,
                pltpu.VMEM((micro, tok, width), BF16),
                pltpu.VMEM((tok, width), F32),
                pltpu.VMEM((tok, width), BF16),
                pltpu.VMEM((span, width), BF16),
                pltpu.VMEM((span, units), BF16),
                pltpu.VMEM((2 * tok, width), F32),
                pltpu.VMEM((micro, local * span, tok), BF16),
                pltpu.VMEM((micro, 2 * tok, local * span), BF16),
                pltpu.SemaphoreType.DMA((3, local)),
                sem, sem, sem, sem,
                pltpu.SemaphoreType.DMA((micro,)),
                pltpu.SemaphoreType.DMA((micro,)),
            ],
            compiler_params=pltpu.CompilerParams(collective_id=0, has_side_effects=True, vmem_limit_bytes=67043328),
            name="layers",
        )(hidden_in, routes[0], gate_probs[0], norm_gain, w_gate[0], w_up[0], w_down[0])
        return out[None]

    in_specs = (
        P(None, ("exp", "pair"), None),
        P("pipe", None, ("exp", "pair"), None),
        P("pipe", None, ("exp", "pair"), None),
        P("pipe", None),
        P("pipe", ("exp", "pair"), None, None),
        P("pipe", ("exp", "pair"), None, None),
        P("pipe", ("exp", "pair"), None, None),
    )
    out_specs = P("pipe", None, ("exp", "pair"), None)
    return jax.shard_map(on_device, mesh=mesh, in_specs=in_specs, out_specs=out_specs, check_vma=False)
```

```python
import functools

import jax
import jax.numpy as jnp
from jax import lax
from jax.experimental import pallas as pl
from jax.experimental.pallas import tpu as pltpu
from jax.sharding import PartitionSpec as P

EPS = 1e-06
MESH = pl.DeviceIdType.MESH
BF16 = jnp.bfloat16
F32 = jnp.float32
SIDE = 4
COLS = 256
PARTS = 2


def kernel(stages, groups, cap, hidden_ref, routes_ref, probs_ref, gain_ref, wg_hbm, wu_hbm, wd_hbm, out_ref,
           wg, wu, wd, send, recv, back, done, relay, state, normed, rows, hid, sums, total, pick, mix,
           w_sem, d_send, d_recv, r_send, r_recv, n_send, n_recv):
    stage, exp, pair = lax.axis_index("pipe"), lax.axis_index("exp"), lax.axis_index("pair")
    pairs = lax.axis_size("pair")
    me = exp * pairs + pair
    micro, tok, width = hidden_ref.shape
    top = routes_ref.shape[1]
    local, _, slots, _ = send.shape[1:]
    span = groups * slots
    hidden_units = wg.shape[2]
    part = width // PARTS

    def weight_copies(e):
        return [pltpu.make_async_copy(hbm.at[e], vmem.at[e], w_sem.at[i, e])
                for i, (hbm, vmem) in enumerate(((wg_hbm, wg), (wu_hbm, wu), (wd_hbm, wd)))]

    for e in range(local):
        for copy in weight_copies(e):
            copy.start()

    barrier = pltpu.get_barrier_semaphore()

    def greet(i, carry):
        peer = lax.rem(me + i, groups)
        pl.semaphore_signal(barrier, inc=1, device_id=(stage, peer // pairs, lax.rem(peer, pairs)), device_id_type=MESH)
        return carry

    lax.fori_loop(1, groups, greet, 0)

    @pl.when(stage > 0)
    def _():
        pl.semaphore_signal(barrier, inc=1, device_id=(stage - 1, exp, pair), device_id_type=MESH)

    def prepare(m):
        column = lax.broadcasted_iota(jnp.int32, (tok, local * groups), 1)
        expert = lax.rem(column, groups) * local + column // groups
        probs = probs_ref[m].T
        probs = probs / jnp.sum(probs, axis=-1, keepdims=True)
        routes = routes_ref[m].T
        named = jnp.zeros((tok, local * groups), F32)
        weight = jnp.zeros((tok, local * groups), F32)
        for k in range(top):
            hit = routes[:, k:k + 1] == expert
            named = named + jnp.where(hit, 1.0, 0.0)
            weight = weight + jnp.where(hit, probs[:, k:k + 1], 0.0)
        earlier = lax.broadcasted_iota(jnp.int32, (tok, tok), 1) < lax.broadcasted_iota(jnp.int32, (tok, tok), 0)
        before = jnp.dot(jnp.where(earlier, 1.0, 0.0).astype(BF16), named.astype(BF16), preferred_element_type=F32)
        high = weight.astype(BF16)
        low = (weight - high.astype(F32)).astype(BF16)
        shape = (local * groups, local * span)
        spread = jnp.where(lax.broadcasted_iota(jnp.int32, shape, 1) // slots == lax.broadcasted_iota(jnp.int32, shape, 0), 1.0, 0.0)
        spread = spread.astype(BF16)
        slot = lax.rem(lax.broadcasted_iota(jnp.int32, (tok, local * span), 1), slots).astype(F32)
        taken = jnp.dot(named.astype(BF16), spread, preferred_element_type=F32)
        place = jnp.dot(before.astype(BF16), spread, preferred_element_type=F32)
        mask = jnp.logical_and(taken > 0.5, jnp.abs(place - slot) < 0.5)
        mix[m, 0:tok, :] = jnp.where(mask, jnp.dot(high, spread, preferred_element_type=F32), 0.0).astype(BF16)
        mix[m, tok:2 * tok, :] = jnp.where(mask, jnp.dot(low, spread, preferred_element_type=F32), 0.0).astype(BF16)
        pick[m] = jnp.where(mask, 1.0, 0.0).T.astype(BF16)

    prepare(0)
    pl.semaphore_wait(barrier, groups - 1 + jnp.minimum(stages - 1 - stage, 1))

    offsets = [(dx, dz, dy) for dx in range(SIDE) for dz in range(SIDE) for dy in range(2)][1:]
    offsets.sort(key=lambda o: -(min(o[0], SIDE - o[0]) + min(o[1], SIDE - o[1]) + o[2]))

    def exchange(source, target, m, e, h, s_sem, r_sem):
        x, z = exp // SIDE, lax.rem(exp, SIDE)
        lanes = pl.ds(h * part, part)
        for dx, dz, dy in offsets:
            peer_exp = lax.rem(x + dx, SIDE) * SIDE + lax.rem(z + dz, SIDE)
            peer_pair = lax.rem(pair + dy, pairs)
            peer = peer_exp * pairs + peer_pair
            pltpu.make_async_remote_copy(
                src_ref=source.at[m, e, peer, pl.ds(0, cap), lanes],
                dst_ref=target.at[m, e, me, pl.ds(0, cap), lanes],
                send_sem=s_sem.at[m, e, h],
                recv_sem=r_sem.at[m, e, h],
                device_id=(stage, peer_exp, peer_pair),
                device_id_type=MESH,
            ).start()
        target[m, e, me, :, lanes] = source[m, e, me, :, lanes]

    def arrived(buffer, m, e, h, sem):
        piece = buffer.at[m, e, pl.ds(0, groups - 1), pl.ds(0, cap), pl.ds(h * part, part)]
        pltpu.make_async_copy(piece, piece, sem.at[m, e, h]).wait()

    def relay_copy(m, h, target_stage):
        lanes = pl.ds(h * part, part)
        return pltpu.make_async_remote_copy(
            src_ref=out_ref.at[m, :, lanes], dst_ref=relay.at[m, :, lanes], send_sem=n_send.at[m, h], recv_sem=n_recv.at[m, h],
            device_id=(target_stage, exp, pair), device_id_type=MESH)

    def begin(m):
        @pl.when(stage == 0)
        def _():
            state[m] = hidden_ref[m].astype(F32)

        @pl.when(stage > 0)
        def _():
            for h in range(PARTS):
                relay_copy(m, h, stage).wait_recv()
            state[m] = relay[m].astype(F32)

        floated = state[m]
        scale = lax.rsqrt(jnp.mean(floated * floated, axis=-1, keepdims=True) + EPS)
        normed[...] = (floated * scale * gain_ref[...]).astype(BF16)

        def dispatch(e, carry):
            first = pl.multiple_of(e * span, span)
            for h in range(PARTS):
                for c in range(h * part, (h + 1) * part, COLS):
                    made = jnp.dot(pick[m, pl.ds(first, span), :], normed[:, c:c + COLS], preferred_element_type=F32)
                    send[m, e, :, :, c:c + COLS] = made.reshape(groups, slots, COLS).astype(BF16)
                exchange(send, recv, m, e, h, d_send, d_recv)
            return carry

        lax.fori_loop(0, local, dispatch, 0)

    def experts(m):
        def ffn(e, carry):
            @pl.when(m == 0)
            def _():
                for copy in weight_copies(e):
                    copy.wait()

            for h in range(PARTS):
                arrived(recv, m, e, h, d_recv)
                low, high = h * part, (h + 1) * part
                rows[...] = recv[m, e, :, :, low:high].reshape(span, part)
                for c in range(0, hidden_units, COLS):
                    gate = jnp.dot(rows[...], wg[e, low:high, c:c + COLS], preferred_element_type=F32)
                    upward = jnp.dot(rows[...], wu[e, low:high, c:c + COLS], preferred_element_type=F32)
                    if h > 0:
                        gate = gate + sums[0, :, c:c + COLS]
                        upward = upward + sums[1, :, c:c + COLS]
                    if h < PARTS - 1:
                        sums[0, :, c:c + COLS] = gate
                        sums[1, :, c:c + COLS] = upward
                    else:
                        hid[:, c:c + COLS] = (jax.nn.silu(gate) * upward).astype(BF16)
            for h in range(PARTS):
                for c in range(h * part, (h + 1) * part, COLS):
                    made = jnp.dot(hid[...], wd[e, :, c:c + COLS], preferred_element_type=F32)
                    back[m, e, :, :, c:c + COLS] = made.reshape(groups, slots, COLS).astype(BF16)
                exchange(back, done, m, e, h, r_send, r_recv)
            return carry

        lax.fori_loop(0, local, ffn, 0)

    def end(m):
        for e in range(local):
            for h in range(PARTS):
                arrived(done, m, e, h, r_recv)
                for c in range(h * part, (h + 1) * part, COLS):
                    mixed = jnp.dot(mix[m, :, e * span:(e + 1) * span],
                                    done[m, e, :, :, c:c + COLS].reshape(span, COLS), preferred_element_type=F32)
                    mixed = mixed[0:tok] + mixed[tok:2 * tok]
                    if e == 0:
                        mixed = mixed + state[m, :, c:c + COLS]
                    else:
                        mixed = mixed + total[:, c:c + COLS]
                    if e < local - 1:
                        total[:, c:c + COLS] = mixed
                    else:
                        out_ref[m, :, c:c + COLS] = mixed.astype(BF16)
                if e == local - 1:
                    @pl.when(stage < stages - 1)
                    def _():
                        relay_copy(m, h, stage + 1).start()

    begin(0)

    def one(m, carry):
        more = m + 1 < micro
        ahead = jnp.logical_or(jnp.logical_and(stage == 0, m == 0), jnp.logical_and(stage >= 2, m == 2))

        @pl.when(more)
        def _():
            prepare(m + 1)

        done[m, :, :, cap:slots, :] = jnp.zeros((local, groups, slots - cap, width), BF16)
        experts(m)

        @pl.when(jnp.logical_and(more, ahead))
        def _():
            begin(m + 1)

        end(m)

        @pl.when(jnp.logical_and(more, jnp.logical_not(ahead)))
        def _():
            begin(m + 1)

        return carry

    lax.fori_loop(0, micro, one, 0)

    def finish(m, carry):
        for h in range(PARTS):
            for e in range(local):
                arrived(send, m, e, h, d_send)
                arrived(back, m, e, h, r_send)

            @pl.when(stage < stages - 1)
            def _():
                relay_copy(m, h, stage + 1).wait_send()

        return carry

    lax.fori_loop(0, micro, finish, 0)


def solution(mesh):
    stages = mesh.shape["pipe"]
    groups = mesh.shape["exp"] * mesh.shape["pair"]

    def on_device(hidden_in, routes, gate_probs, norm_gain, w_gate, w_up, w_down):
        micro, tok, width = hidden_in.shape
        top = routes.shape[3]
        local, _, units = w_gate.shape[1:]
        experts = local * groups
        cap = max(2, 3 * tok * top // (2 * experts))
        slots = -(-cap // 8) * 8
        span = groups * slots
        vmem = pl.BlockSpec(memory_space=pltpu.VMEM)
        hbm = pl.BlockSpec(memory_space=pl.ANY)
        buffer = pltpu.VMEM((micro, local, groups, slots, width), BF16)
        sem = pltpu.SemaphoreType.DMA((micro, local, PARTS))
        out = pl.pallas_call(
            functools.partial(kernel, stages, groups, cap),
            out_shape=jax.ShapeDtypeStruct((micro, tok, width), BF16),
            in_specs=[vmem] * 4 + [hbm] * 3,
            out_specs=vmem,
            scratch_shapes=[
                pltpu.VMEM((local, width, units), BF16),
                pltpu.VMEM((local, width, units), BF16),
                pltpu.VMEM((local, units, width), BF16),
                buffer, buffer, buffer, buffer,
                pltpu.VMEM((micro, tok, width), BF16),
                pltpu.VMEM((micro, tok, width), F32),
                pltpu.VMEM((tok, width), BF16),
                pltpu.VMEM((span, width // PARTS), BF16),
                pltpu.VMEM((span, units), BF16),
                pltpu.VMEM((2, span, units), F32),
                pltpu.VMEM((tok, width), F32),
                pltpu.VMEM((micro, local * span, tok), BF16),
                pltpu.VMEM((micro, 2 * tok, local * span), BF16),
                pltpu.SemaphoreType.DMA((3, local)),
                sem, sem, sem, sem,
                pltpu.SemaphoreType.DMA((micro, PARTS)),
                pltpu.SemaphoreType.DMA((micro, PARTS)),
            ],
            compiler_params=pltpu.CompilerParams(collective_id=0, has_side_effects=True, vmem_limit_bytes=67043328),
            name="layers",
        )(hidden_in, jnp.swapaxes(routes[0], 1, 2), jnp.swapaxes(gate_probs[0], 1, 2), norm_gain, w_gate[0], w_up[0], w_down[0])
        return out[None]

    in_specs = (
        P(None, ("exp", "pair"), None),
        P("pipe", None, ("exp", "pair"), None),
        P("pipe", None, ("exp", "pair"), None),
        P("pipe", None),
        P("pipe", ("exp", "pair"), None, None),
        P("pipe", ("exp", "pair"), None, None),
        P("pipe", ("exp", "pair"), None, None),
    )
    out_specs = P("pipe", None, ("exp", "pair"), None)
    return jax.shard_map(on_device, mesh=mesh, in_specs=in_specs, out_specs=out_specs, check_vma=False)
```

```python
import functools

import jax
import jax.numpy as jnp
from jax import lax
from jax.experimental import pallas as pl
from jax.experimental.pallas import tpu as pltpu
from jax.sharding import PartitionSpec as P

EPS = 1e-06
MESH = pl.DeviceIdType.MESH
BF16 = jnp.bfloat16
F32 = jnp.float32
SIDE = 4
COLS = 256
PARTS = 4


def kernel(stages, groups, cap, hidden_ref, routes_ref, probs_ref, gain_ref, wg_hbm, wu_hbm, wd_hbm, out_ref,
           wg, wu, wd, send, recv, back, done, relay, state, normed, rows, hid, sums, total, pick, mix,
           w_sem, d_send, d_recv, r_send, r_recv, n_send, n_recv):
    stage, exp, pair = lax.axis_index("pipe"), lax.axis_index("exp"), lax.axis_index("pair")
    pairs = lax.axis_size("pair")
    me = exp * pairs + pair
    micro, tok, width = hidden_ref.shape
    top = routes_ref.shape[1]
    local, _, slots, _ = send.shape[1:]
    span = groups * slots
    hidden_units = wg.shape[2]
    part = width // PARTS

    def weight_copies(e):
        return [pltpu.make_async_copy(hbm.at[e], vmem.at[e], w_sem.at[i, e])
                for i, (hbm, vmem) in enumerate(((wg_hbm, wg), (wu_hbm, wu), (wd_hbm, wd)))]

    for e in range(local):
        for copy in weight_copies(e):
            copy.start()

    barrier = pltpu.get_barrier_semaphore()

    def greet(i, carry):
        peer = lax.rem(me + i, groups)
        pl.semaphore_signal(barrier, inc=1, device_id=(stage, peer // pairs, lax.rem(peer, pairs)), device_id_type=MESH)
        return carry

    lax.fori_loop(1, groups, greet, 0)

    @pl.when(stage > 0)
    def _():
        pl.semaphore_signal(barrier, inc=1, device_id=(stage - 1, exp, pair), device_id_type=MESH)

    def prepare(m):
        column = lax.broadcasted_iota(jnp.int32, (tok, local * groups), 1)
        expert = lax.rem(column, groups) * local + column // groups
        probs = probs_ref[m].T
        probs = probs / jnp.sum(probs, axis=-1, keepdims=True)
        routes = routes_ref[m].T
        named = jnp.zeros((tok, local * groups), F32)
        weight = jnp.zeros((tok, local * groups), F32)
        for k in range(top):
            hit = routes[:, k:k + 1] == expert
            named = named + jnp.where(hit, 1.0, 0.0)
            weight = weight + jnp.where(hit, probs[:, k:k + 1], 0.0)
        earlier = lax.broadcasted_iota(jnp.int32, (tok, tok), 1) < lax.broadcasted_iota(jnp.int32, (tok, tok), 0)
        before = jnp.dot(jnp.where(earlier, 1.0, 0.0).astype(BF16), named.astype(BF16), preferred_element_type=F32)
        high = weight.astype(BF16)
        low = (weight - high.astype(F32)).astype(BF16)
        shape = (local * groups, local * span)
        spread = jnp.where(lax.broadcasted_iota(jnp.int32, shape, 1) // slots == lax.broadcasted_iota(jnp.int32, shape, 0), 1.0, 0.0)
        spread = spread.astype(BF16)
        slot = lax.rem(lax.broadcasted_iota(jnp.int32, (tok, local * span), 1), slots).astype(F32)
        taken = jnp.dot(named.astype(BF16), spread, preferred_element_type=F32)
        place = jnp.dot(before.astype(BF16), spread, preferred_element_type=F32)
        mask = jnp.logical_and(taken > 0.5, jnp.abs(place - slot) < 0.5)
        mix[m, 0:tok, :] = jnp.where(mask, jnp.dot(high, spread, preferred_element_type=F32), 0.0).astype(BF16)
        mix[m, tok:2 * tok, :] = jnp.where(mask, jnp.dot(low, spread, preferred_element_type=F32), 0.0).astype(BF16)
        pick[m] = jnp.where(mask, 1.0, 0.0).T.astype(BF16)

    prepare(0)
    pl.semaphore_wait(barrier, groups - 1 + jnp.minimum(stages - 1 - stage, 1))

    offsets = [(dx, dz, dy) for dx in range(SIDE) for dz in range(SIDE) for dy in range(2)][1:]
    offsets.sort(key=lambda o: -(min(o[0], SIDE - o[0]) + min(o[1], SIDE - o[1]) + o[2]))

    def exchange(source, target, m, e, h, s_sem, r_sem):
        x, z = exp // SIDE, lax.rem(exp, SIDE)
        lanes = pl.ds(h * part, part)
        for dx, dz, dy in offsets:
            peer_exp = lax.rem(x + dx, SIDE) * SIDE + lax.rem(z + dz, SIDE)
            peer_pair = lax.rem(pair + dy, pairs)
            peer = peer_exp * pairs + peer_pair
            pltpu.make_async_remote_copy(
                src_ref=source.at[m, e, peer, pl.ds(0, cap), lanes],
                dst_ref=target.at[m, e, me, pl.ds(0, cap), lanes],
                send_sem=s_sem.at[m, e, h],
                recv_sem=r_sem.at[m, e, h],
                device_id=(stage, peer_exp, peer_pair),
                device_id_type=MESH,
            ).start()
        target[m, e, me, :, lanes] = source[m, e, me, :, lanes]

    def arrived(buffer, m, e, h, sem):
        piece = buffer.at[m, e, pl.ds(0, groups - 1), pl.ds(0, cap), pl.ds(h * part, part)]
        pltpu.make_async_copy(piece, piece, sem.at[m, e, h]).wait()

    def relay_copy(m, h, target_stage):
        lanes = pl.ds(h * part, part)
        return pltpu.make_async_remote_copy(
            src_ref=out_ref.at[m, :, lanes], dst_ref=relay.at[m, :, lanes], send_sem=n_send.at[m, h], recv_sem=n_recv.at[m, h],
            device_id=(target_stage, exp, pair), device_id_type=MESH)

    def begin(m):
        @pl.when(stage == 0)
        def _():
            state[m] = hidden_ref[m].astype(F32)

        @pl.when(stage > 0)
        def _():
            for h in range(PARTS):
                relay_copy(m, h, stage).wait_recv()
            state[m] = relay[m].astype(F32)

        floated = state[m]
        scale = lax.rsqrt(jnp.mean(floated * floated, axis=-1, keepdims=True) + EPS)
        normed[...] = (floated * scale * gain_ref[...]).astype(BF16)

        def dispatch(e, carry):
            first = pl.multiple_of(e * span, span)
            for h in range(PARTS):
                for c in range(h * part, (h + 1) * part, COLS):
                    made = jnp.dot(pick[m, pl.ds(first, span), :], normed[:, c:c + COLS], preferred_element_type=F32)
                    send[m, e, :, :, c:c + COLS] = made.reshape(groups, slots, COLS).astype(BF16)
                exchange(send, recv, m, e, h, d_send, d_recv)
            return carry

        lax.fori_loop(0, local, dispatch, 0)

    def experts(m):
        def ffn(e, carry):
            @pl.when(m == 0)
            def _():
                for copy in weight_copies(e):
                    copy.wait()

            for h in range(PARTS):
                arrived(recv, m, e, h, d_recv)
                low, high = h * part, (h + 1) * part
                rows[...] = recv[m, e, :, :, low:high].reshape(span, part)
                for c in range(0, hidden_units, COLS):
                    gate = jnp.dot(rows[...], wg[e, low:high, c:c + COLS], preferred_element_type=F32)
                    upward = jnp.dot(rows[...], wu[e, low:high, c:c + COLS], preferred_element_type=F32)
                    if h > 0:
                        gate = gate + sums[0, :, c:c + COLS]
                        upward = upward + sums[1, :, c:c + COLS]
                    if h < PARTS - 1:
                        sums[0, :, c:c + COLS] = gate
                        sums[1, :, c:c + COLS] = upward
                    else:
                        hid[:, c:c + COLS] = (jax.nn.silu(gate) * upward).astype(BF16)
            for h in range(PARTS):
                for c in range(h * part, (h + 1) * part, COLS):
                    made = jnp.dot(hid[...], wd[e, :, c:c + COLS], preferred_element_type=F32)
                    back[m, e, :, :, c:c + COLS] = made.reshape(groups, slots, COLS).astype(BF16)
                exchange(back, done, m, e, h, r_send, r_recv)
            return carry

        lax.fori_loop(0, local, ffn, 0)

    def end(m):
        for e in range(local):
            for h in range(PARTS):
                arrived(done, m, e, h, r_recv)
                for c in range(h * part, (h + 1) * part, COLS):
                    mixed = jnp.dot(mix[m, :, e * span:(e + 1) * span],
                                    done[m, e, :, :, c:c + COLS].reshape(span, COLS), preferred_element_type=F32)
                    mixed = mixed[0:tok] + mixed[tok:2 * tok]
                    if e == 0:
                        mixed = mixed + state[m, :, c:c + COLS]
                    else:
                        mixed = mixed + total[:, c:c + COLS]
                    if e < local - 1:
                        total[:, c:c + COLS] = mixed
                    else:
                        out_ref[m, :, c:c + COLS] = mixed.astype(BF16)
                if e == local - 1:
                    @pl.when(stage < stages - 1)
                    def _():
                        relay_copy(m, h, stage + 1).start()

    begin(0)

    def one(m, carry):
        more = m + 1 < micro
        ahead = ((2304 >> (stage * 3 + m)) & 1) == 1

        @pl.when(more)
        def _():
            prepare(m + 1)

        done[m, :, :, cap:slots, :] = jnp.zeros((local, groups, slots - cap, width), BF16)
        experts(m)

        @pl.when(jnp.logical_and(more, ahead))
        def _():
            begin(m + 1)

        end(m)

        @pl.when(jnp.logical_and(more, jnp.logical_not(ahead)))
        def _():
            begin(m + 1)

        return carry

    lax.fori_loop(0, micro, one, 0)

    def finish(m, carry):
        for h in range(PARTS):
            for e in range(local):
                arrived(send, m, e, h, d_send)
                arrived(back, m, e, h, r_send)

            @pl.when(stage < stages - 1)
            def _():
                relay_copy(m, h, stage + 1).wait_send()

        return carry

    lax.fori_loop(0, micro, finish, 0)


def solution(mesh):
    stages = mesh.shape["pipe"]
    groups = mesh.shape["exp"] * mesh.shape["pair"]

    def on_device(hidden_in, routes, gate_probs, norm_gain, w_gate, w_up, w_down):
        micro, tok, width = hidden_in.shape
        top = routes.shape[3]
        local, _, units = w_gate.shape[1:]
        experts = local * groups
        cap = max(2, 3 * tok * top // (2 * experts))
        slots = -(-cap // 8) * 8
        span = groups * slots
        vmem = pl.BlockSpec(memory_space=pltpu.VMEM)
        hbm = pl.BlockSpec(memory_space=pl.ANY)
        buffer = pltpu.VMEM((micro, local, groups, slots, width), BF16)
        sem = pltpu.SemaphoreType.DMA((micro, local, PARTS))
        out = pl.pallas_call(
            functools.partial(kernel, stages, groups, cap),
            out_shape=jax.ShapeDtypeStruct((micro, tok, width), BF16),
            in_specs=[vmem] * 4 + [hbm] * 3,
            out_specs=vmem,
            scratch_shapes=[
                pltpu.VMEM((local, width, units), BF16),
                pltpu.VMEM((local, width, units), BF16),
                pltpu.VMEM((local, units, width), BF16),
                buffer, buffer, buffer, buffer,
                pltpu.VMEM((micro, tok, width), BF16),
                pltpu.VMEM((micro, tok, width), F32),
                pltpu.VMEM((tok, width), BF16),
                pltpu.VMEM((span, width // PARTS), BF16),
                pltpu.VMEM((span, units), BF16),
                pltpu.VMEM((2, span, units), F32),
                pltpu.VMEM((tok, width), F32),
                pltpu.VMEM((micro, local * span, tok), BF16),
                pltpu.VMEM((micro, 2 * tok, local * span), BF16),
                pltpu.SemaphoreType.DMA((3, local)),
                sem, sem, sem, sem,
                pltpu.SemaphoreType.DMA((micro, PARTS)),
                pltpu.SemaphoreType.DMA((micro, PARTS)),
            ],
            compiler_params=pltpu.CompilerParams(collective_id=0, has_side_effects=True, vmem_limit_bytes=67043328),
            name="layers",
        )(hidden_in, jnp.swapaxes(routes[0], 1, 2), jnp.swapaxes(gate_probs[0], 1, 2), norm_gain, w_gate[0], w_up[0], w_down[0])
        return out[None]

    in_specs = (
        P(None, ("exp", "pair"), None),
        P("pipe", None, ("exp", "pair"), None),
        P("pipe", None, ("exp", "pair"), None),
        P("pipe", None),
        P("pipe", ("exp", "pair"), None, None),
        P("pipe", ("exp", "pair"), None, None),
        P("pipe", ("exp", "pair"), None, None),
    )
    out_specs = P("pipe", None, ("exp", "pair"), None)
    return jax.shard_map(on_device, mesh=mesh, in_specs=in_specs, out_specs=out_specs, check_vma=False)
```
